32 devices in a mesh: dp: 8 (over z, y), tensor: 4 (over x, core).
Axes of the slice: x: 2, y: 2, z: 4, core: 2. Of those that a mesh axis runs over, the one named last changes fastest.
Arguments:
- hidden: bfloat16 [128, 4096], P(('dp', 'tensor')), may hold values from -6 to 6
- shortcut: bfloat16 [128, 4096], P('dp'), may hold values from -6 to 6
- expert_ids: int32 [128, 2], P('dp'), may hold values from 0 to 7, all different within a row; in each aligned block of 16 rows (0 to 15, 16 to 31, ...) at most 6 rows name the same one
- route_weight: float32 [128, 2], P('dp'), may hold values from 0.1 to 1
- dense_gain: float32 [4096], replicated, may hold values from 0.5 to 1.5
- moe_gain: float32 [4096], replicated, may hold values from 0.5 to 1.5
- dense_gate: bfloat16 [4096, 8192], P(None, 'dp'), may hold values from -0.09375 to 0.09375
- dense_lift: bfloat16 [4096, 8192], P(None, 'dp'), may hold values from -0.09375 to 0.09375
- dense_down: bfloat16 [8192, 4096], P('dp'), may hold values from -0.0625 to 0.0625
- expert_gate: bfloat16 [4096, 65536], P(None, ('dp', 'tensor')), may hold values from -0.09375 to 0.09375
- expert_lift: bfloat16 [4096, 65536], P(None, ('dp', 'tensor')), may hold values from -0.09375 to 0.09375
- expert_down: bfloat16 [65536, 4096], P(('dp', 'tensor')), may hold values from -0.0625 to 0.0625
Outputs:
- mixed: bfloat16 [128, 4096], P(('dp', 'tensor'))
The draws below stay inside these ranges and needn't reach their ends.
Inputs may be any that keep to these rules, and one draw needn't show every extreme that they name: `expert_ids`: the 2 experts of a token differ. In each aligned block of 16 rows (the tokens of one index of dp) no expert is named by more than 6 rows, and in every draw some expert is named by exactly 6 rows of some block; every expert is named somewhere.
All inputs are finite; a program needn't handle non-finite values.
Results may differ from the reference program's by a relative error of at most 0.006.
Values may be sent and summed in bfloat16 or wider, within the bound.
A program may use at most 128 MiB of HBM per device.

```python
import math
import jax
import jax.numpy as jnp
import numpy as np
from jax import lax

D = 4096
E = 8
TOP = 2
FF = 8192
FF_E = 8192
TOK_DEV = 16
CAP = 6
SLICE = 2048
TOKENS = 128


def shard_levels(key, extent, split, smallest, largest):
    def one(axis_at, blocks):
        heights = jax.random.uniform(jax.random.fold_in(jax.random.fold_in(key, 6), axis_at), (blocks,), jnp.float32, smallest / len(split), largest / len(split))
        return jnp.repeat(jnp.exp(heights), extent[axis_at] // blocks).reshape((-1,) + (1,) * (len(extent) - axis_at - 1))

    level = one(*split[0])
    for cut in split[1:]:
        level = level * one(*cut)
    return level


def deal_out(key, own, number, rows, amount, top, limit, lean):
    sequence = jax.random.permutation(key, amount)
    packed, usual = portions_of(amount, rows * top, limit, lean, True), portions_of(amount, rows * top, limit, lean, False)
    places = jnp.arange(amount)

    def named(lengths, offset_by):
        used = int((lengths > 0).sum())
        fixed = max(1, used // 4)
        shifted = fixed + (places - fixed + offset_by * (used - fixed)) % max(1, amount - fixed)
        return jnp.zeros((amount,), jnp.int32).at[sequence[jnp.where(places < fixed, places, shifted)]].set(jnp.asarray(lengths, jnp.int32))

    lengths = jnp.where(number % 4 == 0, named(packed, number // 4), named(usual, number - number // 4 - 1))
    mixed = jax.random.permutation(jax.random.fold_in(own, 3), amount)
    giver, sink = mixed[0:amount // 2 * 2:2], mixed[1:amount // 2 * 2:2]
    margin = jnp.minimum(lengths[giver] - 1, limit - lengths[sink]) // 2
    margin = jnp.where((giver == sequence[0]) | (sink == sequence[0]) | (lengths[sink] == 0), 0, jnp.maximum(margin, 0))
    shifted = jax.random.randint(jax.random.fold_in(own, 4), (amount // 2,), 0, 1 << 20) % (margin + 1)
    lengths = lengths.at[giver].add(-shifted).at[sink].add(shifted)
    items = jnp.searchsorted(jnp.cumsum(lengths), jnp.arange(rows * top), side="right").astype(jnp.int32)
    grid = items.reshape(top, rows).T
    grid = grid[jax.random.permutation(jax.random.fold_in(own, 1), rows)]
    offset_by = jax.random.randint(jax.random.fold_in(own, 2), (rows, 1), 0, top)
    return jnp.take_along_axis(grid, (jnp.arange(top)[None, :] + offset_by) % top, axis=1)


def portions_of(number_of, total, most, slope, full):
    weights = [(1 << 20) // math.isqrt(grade ** slope) + 1 for grade in range(1, number_of + 1)]
    largest = most if full else min(most, max(-(-total // number_of), total * weights[0] // sum(weights)))
    least = 1 if total - largest >= number_of - 1 else 0
    counts, surplus = [largest] + [least] * (number_of - 1), total - largest - least * (number_of - 1)
    while surplus > 0:
        movable = [i for i in range(1, number_of) if counts[i] < largest] or [i for i in range(1, number_of) if counts[i] < most]
        pool, remaining = sum([weights[i] for i in movable]), surplus
        for i in movable:
            extra = min(most - counts[i], max(1, remaining * weights[i] // pool), surplus)
            counts[i] = counts[i] + extra
            surplus = surplus - extra
    return np.array(counts)


def scatter_about(own_key, extent, scale, limit, split=(), kind=jnp.bfloat16):
    array = jax.random.normal(own_key, extent, jnp.float32) * scale
    if len(split) > 0:
        array = shard_levels(own_key, extent, split, -0.22, 0.18) * array
    return jnp.clip(array, min=-limit, max=limit).astype(kind)


def setup_inputs(seed: int = 0) -> dict:
    splits = jax.random.split(jax.random.key(seed), 13)
    hidden = scatter_about(splits[0], (TOKENS, D), 1.0, 6.0, ((0, 32),))
    shortcut = scatter_about(splits[1], (TOKENS, D), 1.0, 6.0, ((0, 8),))
    expert_ids_keys = jax.random.split(jax.random.fold_in(splits[2], 1), TOKENS // TOK_DEV)
    expert_ids_turns = jax.random.permutation(jax.random.fold_in(splits[2], 3), TOKENS // TOK_DEV)
    expert_ids = jax.vmap(lambda own, number: deal_out(jax.random.fold_in(splits[2], 2), own, number, TOK_DEV, E, TOP, CAP, 2))(expert_ids_keys, expert_ids_turns).reshape((TOKENS, TOP))
    route_weight = jnp.clip(0.1 + 0.9 * jax.random.uniform(splits[3], (TOKENS, TOP), jnp.float32) ** shard_levels(splits[3], (TOKENS, TOP), ((0, 8),), -0.2, 0.2), 0.1, 1.0)
    dense_gain = jnp.clip(jax.random.uniform(splits[4], (D,), jnp.float32, 0.5, 1.5), 0.5, 1.5)
    moe_gain = jnp.clip(jax.random.uniform(splits[5], (D,), jnp.float32, 0.5, 1.5), 0.5, 1.5)
    dense_gate = scatter_about(splits[6], (D, FF), D ** -0.5, 0.09375, ((1, 8),))
    dense_lift = scatter_about(splits[7], (D, FF), D ** -0.5, 0.09375, ((1, 8),))
    dense_down = scatter_about(splits[8], (FF, D), FF ** -0.5, 0.0625, ((0, 8),))
    expert_gate = scatter_about(splits[9], (D, E * FF_E), D ** -0.5, 0.09375, ((1, 32),))
    expert_lift = scatter_about(splits[10], (D, E * FF_E), D ** -0.5, 0.09375, ((1, 32),))
    expert_down = scatter_about(splits[11], (E * FF_E, D), FF_E ** -0.5, 0.0625, ((0, 32),))
    return {"hidden": hidden, "shortcut": shortcut, "expert_ids": expert_ids, "route_weight": route_weight, "dense_gain": dense_gain, "moe_gain": moe_gain, "dense_gate": dense_gate, "dense_lift": dense_lift, "dense_down": dense_down, "expert_gate": expert_gate, "expert_lift": expert_lift, "expert_down": expert_down}


EPSILON = 1e-05

def normalize(values_in, gain):
    values = values_in.astype(jnp.float32)
    scale = lax.rsqrt(lax.optimization_barrier(jnp.mean(values * values, axis=-1, keepdims=True)) + EPSILON)
    return (values * scale * gain).astype(jnp.bfloat16)

def slot_places(expert_ids):
    blocks = expert_ids.shape[0] // TOK_DEV
    flat = expert_ids.reshape(blocks, TOK_DEV * TOP)
    picked = (flat[:, :, None] == jnp.arange(E, dtype=jnp.int32)[None, None, :]).astype(jnp.int32)
    before = jnp.cumsum(picked, axis=1) - picked
    ranks = lax.optimization_barrier(jnp.sum(before * picked, axis=2))
    return flat * CAP + ranks

def reference(hidden, shortcut, expert_ids, route_weight, dense_gain, moe_gain, dense_gate, dense_lift, dense_down, expert_gate, expert_lift, expert_down):
    normed = normalize(hidden, dense_gain)
    gate_vals = jnp.dot(normed, dense_gate, preferred_element_type=jnp.float32)
    lift_vals = jnp.dot(normed, dense_lift, preferred_element_type=jnp.float32)
    dense_inner = (jax.nn.silu(gate_vals) * lift_vals).astype(jnp.bfloat16)
    dense_out = jnp.dot(dense_inner, dense_down, preferred_element_type=jnp.float32)
    moe_in = normalize(shortcut, moe_gain)
    blocks = TOKENS // TOK_DEV
    places = slot_places(expert_ids)
    chosen = (places[:, :, None] == jnp.arange(E * CAP, dtype=jnp.int32)[None, None, :]).astype(jnp.float32)
    chosen = chosen.reshape(blocks, TOK_DEV, TOP, E * CAP)
    spread = lax.optimization_barrier(jnp.sum(chosen, axis=2))
    weighted = lax.optimization_barrier(jnp.sum(chosen * route_weight.reshape(blocks, TOK_DEV, TOP, 1), axis=2))
    grouped = moe_in.astype(jnp.float32).reshape(blocks, TOK_DEV, D)
    buffer = jnp.einsum('bts,btd->bsd', spread, grouped).astype(jnp.bfloat16).reshape(blocks, E, CAP, D)
    parts = FF_E // SLICE

    def one_expert(expert):
        rows_in = lax.dynamic_index_in_dim(buffer, expert, 1, keepdims=False).reshape(blocks * CAP, D)
        start = expert * FF_E
        gate_part = jnp.dot(rows_in, lax.dynamic_slice_in_dim(expert_gate, start, FF_E, 1), preferred_element_type=jnp.float32)
        lift_part = jnp.dot(rows_in, lax.dynamic_slice_in_dim(expert_lift, start, FF_E, 1), preferred_element_type=jnp.float32)
        inner = (jax.nn.silu(gate_part) * lift_part).astype(jnp.bfloat16)

        def add_part(total, index):
            first = index * SLICE
            term = jnp.dot(lax.dynamic_slice_in_dim(inner, first, SLICE, 1), lax.dynamic_slice_in_dim(expert_down, start + first, SLICE, 0), preferred_element_type=jnp.float32).astype(jnp.bfloat16)
            term = lax.optimization_barrier(term)
            return (total + term.astype(jnp.float32), None)
        return lax.scan(add_part, jnp.zeros((blocks * CAP, D), jnp.float32), jnp.arange(parts, dtype=jnp.int32))[0]
    outputs = lax.map(one_expert, jnp.arange(E, dtype=jnp.int32))
    outputs = outputs.reshape(E, blocks, CAP, D).transpose(1, 0, 2, 3).reshape(blocks, E * CAP, D)
    moe_out = jnp.einsum('bts,bsd->btd', weighted, outputs, precision=lax.Precision.HIGHEST).reshape(TOKENS, D)
    return (hidden.astype(jnp.float32) + dense_out + moe_out).astype(jnp.bfloat16)
```

```python
import functools

import jax
import jax.numpy as jnp
from jax import lax
from jax.experimental import pallas as pl
from jax.experimental.pallas import tpu as pltpu
from jax.sharding import PartitionSpec as P

E = 8
TOP = 2
CAP = 6
CP = 8
NQ = 2
EPSILON = 1e-05
MESH = pl.DeviceIdType.MESH
F32 = jnp.float32
BF16 = jnp.bfloat16


def rms_scale(values):
    return lax.rsqrt(jnp.mean(values * values, axis=-1, keepdims=True) + EPSILON)


def each(lo, hi, body):
    if hi - lo <= 8:
        for k in range(lo, hi):
            body(k)
    else:
        def step(k, _):
            body(k)
            return 0

        lax.fori_loop(lo, hi, step, 0)


def silu_mul(g, v):
    return (g / (1.0 + jnp.exp(-g)) * v).astype(BF16)


def kernel(
    cfg,
    hidden, shortcut, ids, route, dgain, mgain, dg, dl, dd, eg, el, ed,
    out,
    pool, epool, dgp, dlp, ddp,
    disp, land, xe, accg, accl, inner_e,
    ag, stage, xd, inner_d, own, part, pland, ds, dland,
    rs, rsland, ret, retland, fin, finland,
    wsem, esem, dsem,
    di_s, di_r, pd_s, pd_r, ag_s, ag_r, px_s, px_r,
    pr_s, pr_r, re_s, re_r, po_s, po_r, ds_s, ds_r, fi_s, fi_r,
):
    np_, nt, sp, reuse = cfg
    h, D = hidden.shape
    B = shortcut.shape[0]
    fe = eg.shape[1]
    fd = dg.shape[1] // sp
    Dh = D // 2
    kc = Dh // NQ
    nk = 2 * NQ
    dc = D // 2
    members = np_ // E
    rows = np_ * CP
    p = lax.axis_index("dp")
    t = lax.axis_index("tensor")
    c = lax.rem(t, 2)
    mate = t + 1 - 2 * c

    def half(k):
        return c if k < NQ else 1 - c

    def k_rows(k):
        return pl.ds(pl.multiple_of(half(k) * Dh + (k % NQ) * kc, kc), kc)

    def w_copy(k, which):
        src = (eg, el)[which]
        return pltpu.make_async_copy(src.at[k_rows(k), :], pool.at[2 * k + which], wsem.at[2 * k + which])

    def e_cols(i):
        side = 1 - c if i < NQ else c
        return pl.ds(pl.multiple_of(side * Dh + (i % NQ) * kc, kc), kc)

    def e_copy(i):
        return pltpu.make_async_copy(ed.at[:, e_cols(i)], epool.at[i], esem.at[i])

    dcols = pl.ds(pl.multiple_of((c if sp == 2 else 0) * fd, fd), fd)

    def dense_w(k, which):
        if reuse:
            return pool.at[which, :, k * fd : (k + 1) * fd]
        return (dgp, dlp)[which].at[k]

    def dense_d(i):
        if reuse:
            return pool.at[2, i * fd : (i + 1) * fd, :]
        return ddp.at[i]

    def d_copy(k, which):
        src = (dg, dl)[which]
        return pltpu.make_async_copy(
            src.at[k * kc : (k + 1) * kc, dcols], dense_w(k, which), dsem.at[2 * k + which]
        )

    def dd_copy(i):
        return pltpu.make_async_copy(
            dd.at[dcols, i * dc : (i + 1) * dc], dense_d(i), dsem.at[2 * nk + i]
        )

    barrier = pltpu.get_barrier_semaphore()
    land[...] = jnp.zeros(land.shape, BF16)
    retland[...] = jnp.zeros(retland.shape, BF16)

    def greet(k):
        pl.semaphore_signal(
            barrier, inc=1, device_id=(lax.rem(p + k, np_), t), device_id_type=MESH
        )

    each(1, np_, greet)
    for j in range(1, nt):
        pl.semaphore_signal(
            barrier, inc=1, device_id=(p, lax.rem(t + j, nt)), device_id_type=MESH
        )

    for k in range(nk):
        w_copy(k, 0).start()
        w_copy(k, 1).start()
    for i in range(nk):
        e_copy(i).start()
    if not reuse:
        for k in range(nk):
            d_copy(k, 0).start()
            d_copy(k, 1).start()
        for i in range(2):
            dd_copy(i).start()

    wide = np_ * CP
    col = lax.broadcasted_iota(jnp.int32, (B, max(wide, 128)), 1)

    def places(members):
        col_e = lax.shift_right_logical(col, 3) // members
        at0 = jnp.where(ids[:, 0:1] == col_e, 1.0, 0.0).astype(F32)
        at1 = jnp.where(ids[:, 1:2] == col_e, 1.0, 0.0).astype(F32)
        return at0, at1

    r_i = lax.broadcasted_iota(jnp.int32, (B, B), 0)
    c_i = lax.broadcasted_iota(jnp.int32, (B, B), 1)
    lower = jnp.where(c_i < r_i, 1.0, 0.0).astype(BF16)

    def spread_of(members):
        at0, at1 = places(members)
        named = at0 + at1
        before = jnp.dot(lower, named.astype(BF16), preferred_element_type=F32)
        spread = jnp.where(before.astype(jnp.int32) == (col & 7), named, 0.0)
        return spread, at0, at1

    spread = spread_of(1)[0]
    spread_t = jnp.transpose(spread)[: E * CP].astype(BF16)

    sc = rms_scale(shortcut[...].astype(F32))
    for q in range(NQ):
        mine = pl.ds(pl.multiple_of(c * Dh + q * kc, kc), kc)
        moe_q = (shortcut[:, mine].astype(F32) * sc * mgain[:, mine]).astype(BF16)
        buf = jnp.dot(spread_t, moe_q, preferred_element_type=F32)
        disp[q] = buf.reshape(E, CP, kc).astype(BF16)

    hid = hidden[...].astype(F32)
    ag[p] = (hid * rms_scale(hid) * dgain[...]).astype(BF16)

    real = pl.ds(0, CAP)

    def di_copy(k, q, src):
        to = lax.rem(p + k, np_)
        return pltpu.make_async_remote_copy(
            src_ref=disp.at[q, to // members, real], dst_ref=land.at[c, q, src, real],
            send_sem=di_s.at[q, k], recv_sem=di_r.at[q, src], device_id=(to, t),
            device_id_type=MESH,
        )

    def ag_copy(k, src):
        return pltpu.make_async_remote_copy(
            src_ref=ag.at[src], dst_ref=ag.at[src], send_sem=ag_s.at[k],
            recv_sem=ag_r.at[src], device_id=(lax.rem(p + k, np_), t), device_id_type=MESH,
        )

    def mate_copy(src, dst, send, recv):
        return pltpu.make_async_remote_copy(
            src_ref=src, dst_ref=dst, send_sem=send, recv_sem=recv, device_id=(p, mate),
            device_id_type=MESH,
        )

    pl.semaphore_wait(barrier, np_ + nt - 2)
    for q in range(NQ):
        each(1, np_, lambda k: di_copy(k, q, p).start())
    each(1, np_, lambda k: ag_copy(k, p).start())

    for q in range(NQ):
        land[c, q, p] = disp[q, p // members]

    spread_m, at0, at1 = spread_of(members)
    weighted = spread_m * (at0 * route[:, 0:1] + at1 * route[:, 1:2])
    weighted = weighted[:, :wide]
    w_hi = weighted.astype(BF16)
    w_lo = (weighted - w_hi.astype(F32)).astype(BF16)

    def pd_copy(q, side):
        return mate_copy(land.at[side, q], land.at[side, q], pd_s.at[q], pd_r.at[q])

    nb = max(fe // 512, 1)
    cb = fe // nb
    for k in range(nk):
        q = k % NQ
        if k < NQ:
            each(1, np_, lambda j: di_copy(j, q, lax.rem(p + j, np_)).wait_recv())
            pd_copy(q, c).start()
        else:
            pd_copy(q, 1 - c).wait_recv()
        xe[k] = land[half(k), q].astype(F32).reshape(rows, kc).astype(BF16)
        w_copy(k, 0).wait()
        w_copy(k, 1).wait()
        if k == 0:
            accg[...] = jnp.dot(xe[k], pool[0], preferred_element_type=F32)
            accl[...] = jnp.dot(xe[k], pool[1], preferred_element_type=F32)
        elif k < nk - 1:
            accg[...] = accg[...] + jnp.dot(xe[k], pool[2 * k], preferred_element_type=F32)
            accl[...] = accl[...] + jnp.dot(xe[k], pool[2 * k + 1], preferred_element_type=F32)
        else:
            for b in range(nb):
                cols = slice(b * cb, (b + 1) * cb)
                g = accg[:, cols] + jnp.dot(xe[k], pool[2 * k, :, cols], preferred_element_type=F32)
                v = accl[:, cols] + jnp.dot(xe[k], pool[2 * k + 1, :, cols], preferred_element_type=F32)
                inner_e[:, cols] = silu_mul(g, v)
        if reuse and k == 0:
            for i in range(nk):
                d_copy(i, 0).start()
                d_copy(i, 1).start()
        if reuse and k == 1:
            for i in range(2):
                dd_copy(i).start()

    nh = np_ * h
    me = c if sp == 2 else 0
    each(1, np_, lambda k: ag_copy(k, lax.rem(p + k, np_)).wait_recv())
    for s in range(np_):
        stage[s * h : (s + 1) * h, :] = ag[s].astype(F32)
    xd[me] = stage[...].astype(BF16)
    if sp == 2:
        px = mate_copy(xd.at[me], xd.at[me], px_s.at[0], px_r.at[0])
        px.start()

    def pr_copy(q):
        return mate_copy(rs.at[q], rsland.at[q], pr_s.at[q], pr_r.at[q])

    def re_copy(k, q, src):
        to = lax.rem(p + k, np_)
        return pltpu.make_async_remote_copy(
            src_ref=ret.at[q, to, real], dst_ref=retland.at[q, src, real],
            send_sem=re_s.at[q, k], recv_sem=re_r.at[q, src], device_id=(to, t),
            device_id_type=MESH,
        )

    for i in range(nk):
        q = i % NQ
        e_copy(i).wait()
        o = jnp.dot(inner_e[...], epool[i], preferred_element_type=F32)
        if i < NQ:
            rs[q] = o.reshape(np_, CP, kc).astype(BF16)
            pr_copy(q).start()
        else:
            pr_copy(q).wait_recv()
            ret[q] = (o.reshape(np_, CP, kc) + rsland[q].astype(F32)).astype(BF16)
            each(1, np_, lambda k: re_copy(k, q, p).start())
            retland[q, p] = ret[q, p]

    if sp == 2:
        mate_copy(xd.at[1 - me], xd.at[1 - me], px_s.at[0], px_r.at[0]).wait_recv()
    g = None
    for k in range(nk):
        d_copy(k, 0).wait()
        d_copy(k, 1).wait()
    xk = xd[...].astype(F32).reshape(sp * nh, D).astype(BF16)
    g = v = None
    for k in range(nk):
        lhs = xk[:, k * kc : (k + 1) * kc]
        gk = jnp.dot(lhs, dense_w(k, 0)[...], preferred_element_type=F32)
        vk = jnp.dot(lhs, dense_w(k, 1)[...], preferred_element_type=F32)
        g = gk if g is None else g + gk
        v = vk if v is None else v + vk
    inner_d[...] = silu_mul(g, v)

    def po_copy(i):
        return mate_copy(part.at[i], pland.at[i], po_s.at[i], po_r.at[i])

    def ds_copy(k, i, src):
        to = lax.rem(p + k, np_)
        return pltpu.make_async_remote_copy(
            src_ref=ds.at[i, to], dst_ref=dland.at[i, src], send_sem=ds_s.at[i, k],
            recv_sem=ds_r.at[i, src], device_id=(to, t), device_id_type=MESH,
        )

    for i in range(2):
        dd_copy(i).wait()
        o = jnp.dot(inner_d[...], dense_d(i)[...], preferred_element_type=F32)
        if sp == 2:
            own[i] = jnp.where(c == 0, o[:nh], o[nh:])
            part[i] = jnp.where(c == 0, o[nh:], o[:nh]).astype(BF16)
            po_copy(i).start()
        else:
            own[i] = o
    for i in range(2):
        o = own[i]
        if sp == 2:
            po_copy(i).wait_recv()
            o = o + pland[i].astype(F32)
        for s in range(np_):
            ds[i, s] = o[s * h : (s + 1) * h, :].astype(BF16)
        each(1, np_, lambda k: ds_copy(k, i, p).start())
        dland[i, p] = ds[i, p]

    def fi_copy(j, q, src):
        to = lax.rem(t + j, nt)
        return pltpu.make_async_remote_copy(
            src_ref=fin.at[to, q], dst_ref=finland.at[src, q], send_sem=fi_s.at[j, q],
            recv_sem=fi_r.at[src, q], device_id=(p, to), device_id_type=MESH,
        )

    for q in range(NQ):
        each(1, np_, lambda k: re_copy(k, q, lax.rem(p + k, np_)).wait_recv())
        back = retland[q].astype(F32).reshape(rows, kc).astype(BF16)
        moe = jnp.dot(w_hi, back, preferred_element_type=F32)
        moe = moe + jnp.dot(w_lo, back, preferred_element_type=F32)
        for j in range(nt):
            fin[j, q] = moe[j * h : (j + 1) * h, :].astype(BF16)
        for j in range(1, nt):
            fi_copy(j, q, t).start()
        finland[t, q] = fin[t, q]

    for i in range(2):
        each(1, np_, lambda k: ds_copy(k, i, lax.rem(p + k, np_)).wait_recv())
    for q in range(NQ):
        for j in range(1, nt):
            fi_copy(j, q, lax.rem(t + j, nt)).wait_recv()
    for i in range(2):
        acc = hid[:, i * dc : (i + 1) * dc]
        for s in range(np_):
            acc = acc + dland[i, s].astype(F32)
        for q in range(NQ):
            a = acc[:, q * kc : (q + 1) * kc]
            for j in range(i, nt, 2):
                a = a + finland[j, q].astype(F32)
            out[:, i * Dh + q * kc : i * Dh + (q + 1) * kc] = a.astype(BF16)

    def sent(k):
        for q in range(NQ):
            di_copy(k, q, p).wait_send()
            re_copy(k, q, p).wait_send()
        ag_copy(k, p).wait_send()
        for i in range(2):
            ds_copy(k, i, p).wait_send()

    each(1, np_, sent)
    for q in range(NQ):
        pd_copy(q, c).wait_send()
        pr_copy(q).wait_send()
        for j in range(1, nt):
            fi_copy(j, q, t).wait_send()
    if sp == 2:
        px.wait_send()
        for i in range(2):
            po_copy(i).wait_send()


def local(np_, nt, hidden, shortcut, ids, route, dgain, mgain, dg, dl, dd, eg, el, ed):
    h, D = hidden.shape
    fe = eg.shape[1]
    sp = 2 if dg.shape[1] % 256 == 0 else 1
    fd = dg.shape[1] // sp
    Dh = D // 2
    kc = Dh // NQ
    nk = 2 * NQ
    reuse = nk * fd <= fe and Dh <= fe and 2 * fd <= kc
    nh = np_ * h
    rows = np_ * CP
    dma = pltpu.SemaphoreType.DMA
    vm = pltpu.VMEM
    vspec = pl.BlockSpec(memory_space=pltpu.VMEM)
    aspec = pl.BlockSpec(memory_space=pl.ANY)
    tiny = vm((8, 128), BF16)
    return pl.pallas_call(
        functools.partial(kernel, (np_, nt, sp, reuse)),
        out_shape=jax.ShapeDtypeStruct((h, D), BF16),
        in_specs=[vspec] * 6 + [aspec] * 6,
        out_specs=vspec,
        scratch_shapes=[
            vm((2 * nk, kc, fe), BF16), vm((nk, fe, kc), BF16),
            tiny if reuse else vm((nk, kc, fd), BF16),
            tiny if reuse else vm((nk, kc, fd), BF16),
            tiny if reuse else vm((2, fd, Dh), BF16),
            vm((NQ, E, CP, kc), BF16), vm((2, NQ, np_, CP, kc), BF16), vm((nk, rows, kc), BF16),
            vm((rows, fe), F32), vm((rows, fe), F32), vm((rows, fe), BF16),
            vm((np_, h, D), BF16), vm((nh, D), F32), vm((sp, nh, D), BF16), vm((sp * nh, fd), BF16),
            vm((2, nh, Dh), F32), vm((2, nh, Dh), BF16), vm((2, nh, Dh), BF16),
            vm((2, np_, h, Dh), BF16), vm((2, np_, h, Dh), BF16),
            vm((NQ, np_, CP, kc), BF16), vm((NQ, np_, CP, kc), BF16),
            vm((NQ, np_, CP, kc), BF16), vm((NQ, np_, CP, kc), BF16),
            vm((nt, NQ, h, kc), BF16), vm((nt, NQ, h, kc), BF16),
            dma((2 * nk,)), dma((nk,)), dma((2 * nk + 2,)),
            dma((NQ, np_)), dma((NQ, np_)), dma((NQ,)), dma((NQ,)), dma((np_,)), dma((np_,)),
            dma((1,)), dma((1,)),
            dma((NQ,)), dma((NQ,)), dma((NQ, np_)), dma((NQ, np_)), dma((2,)), dma((2,)),
            dma((2, np_)), dma((2, np_)), dma((nt, NQ)), dma((nt, NQ)),
        ],
        compiler_params=pltpu.CompilerParams(
            collective_id=0, has_side_effects=True, vmem_limit_bytes=64 * 1024 * 1024 - 65536
        ),
    )(hidden, shortcut, ids, route, dgain.reshape(1, D), mgain.reshape(1, D), dg, dl, dd, eg, el, ed)


def solution(mesh):
    in_specs = (
        P(("dp", "tensor"), None),
        P("dp", None),
        P("dp", None),
        P("dp", None),
        P(),
        P(),
        P(None, "dp"),
        P(None, "dp"),
        P("dp", None),
        P(None, ("dp", "tensor")),
        P(None, ("dp", "tensor")),
        P(("dp", "tensor"), None),
    )
    body = functools.partial(local, mesh.shape["dp"], mesh.shape["tensor"])
    return jax.shard_map(
        body, mesh=mesh, in_specs=in_specs, out_specs=P(("dp", "tensor"), None), check_vma=False
    )
```

```python
import functools

import jax
import jax.numpy as jnp
from jax import lax
from jax.experimental import pallas as pl
from jax.experimental.pallas import tpu as pltpu
from jax.sharding import PartitionSpec as P

E = 8
TOP = 2
CAP = 6
CP = 8
NQ = 2
EPSILON = 1e-05
MESH = pl.DeviceIdType.MESH
F32 = jnp.float32
BF16 = jnp.bfloat16


def rms_scale(values):
    return lax.rsqrt(jnp.mean(values * values, axis=-1, keepdims=True) + EPSILON)


def each(lo, hi, body):
    if hi - lo <= 8:
        for k in range(lo, hi):
            body(k)
    else:
        def step(k, _):
            body(k)
            return 0

        lax.fori_loop(lo, hi, step, 0)


def silu_mul(g, v):
    return (g / (1.0 + jnp.exp(-g)) * v).astype(BF16)


def kernel(
    cfg,
    hidden_, shortcut_, ids_, route_, dgain_, mgain_, dg, dl, dd, eg, el, ed,
    out,
    hidden, shortcut, ids, route, dgain, mgain,
    pool, epool, dgp, dlp, ddp,
    disp, land, xe, accg, accl, inner_e,
    ag, stage, xd, inner_d, own, part, pland, ds, dland,
    rs, rsland, ret, retland, fin, finland,
    isem, wsem, esem, dsem,
    di_s, di_r, pd_s, pd_r, ag_s, ag_r, px_s, px_r,
    pr_s, pr_r, re_s, re_r, po_s, po_r, ds_s, ds_r, fi_s, fi_r,
):
    np_, nt, sp, reuse = cfg
    h, D = hidden.shape
    B = shortcut.shape[0]
    fe = eg.shape[1]
    fd = dg.shape[1] // sp
    Dh = D // 2
    kc = Dh // NQ
    nk = 2 * NQ
    dc = D // 2
    members = np_ // E
    rows = np_ * CP
    p = lax.axis_index("dp")
    t = lax.axis_index("tensor")
    c = lax.rem(t, 2)
    mate = t + 1 - 2 * c

    def half(k):
        return c if k < NQ else 1 - c

    def k_rows(k):
        return pl.ds(pl.multiple_of(half(k) * Dh + (k % NQ) * kc, kc), kc)

    def w_copy(k, which):
        src = (eg, el)[which]
        return pltpu.make_async_copy(src.at[k_rows(k), :], pool.at[2 * k + which], wsem.at[2 * k + which])

    def e_cols(i):
        side = 1 - c if i < NQ else c
        return pl.ds(pl.multiple_of(side * Dh + (i % NQ) * kc, kc), kc)

    def e_copy(i):
        return pltpu.make_async_copy(ed.at[:, e_cols(i)], epool.at[i], esem.at[i])

    dcols = pl.ds(pl.multiple_of((c if sp == 2 else 0) * fd, fd), fd)

    def dense_w(k, which):
        if reuse:
            return pool.at[which, :, k * fd : (k + 1) * fd]
        return (dgp, dlp)[which].at[k]

    def dense_d(i):
        if reuse:
            return pool.at[2, i * fd : (i + 1) * fd, :]
        return ddp.at[i]

    def d_copy(k, which):
        src = (dg, dl)[which]
        return pltpu.make_async_copy(
            src.at[k * kc : (k + 1) * kc, dcols], dense_w(k, which), dsem.at[2 * k + which]
        )

    def dd_copy(i):
        return pltpu.make_async_copy(
            dd.at[dcols, i * dc : (i + 1) * dc], dense_d(i), dsem.at[2 * nk + i]
        )

    small = (
        (ids_, ids), (route_, route), (mgain_, mgain), (shortcut_, shortcut), (hidden_, hidden), (dgain_, dgain)
    )
    small = [pltpu.make_async_copy(a, b, isem.at[i]) for i, (a, b) in enumerate(small)]
    for copy in small:
        copy.start()
    barrier = pltpu.get_barrier_semaphore()
    land[...] = jnp.zeros(land.shape, BF16)
    retland[...] = jnp.zeros(retland.shape, BF16)

    def greet(k):
        pl.semaphore_signal(
            barrier, inc=1, device_id=(lax.rem(p + k, np_), t), device_id_type=MESH
        )

    each(1, np_, greet)
    for j in range(1, nt):
        pl.semaphore_signal(
            barrier, inc=1, device_id=(p, lax.rem(t + j, nt)), device_id_type=MESH
        )

    for k in range(nk):
        w_copy(k, 0).start()
        w_copy(k, 1).start()
    for i in range(nk):
        e_copy(i).start()
    if not reuse:
        for k in range(nk):
            d_copy(k, 0).start()
            d_copy(k, 1).start()
        for i in range(2):
            dd_copy(i).start()

    for copy in small:
        copy.wait()
    r_i = lax.broadcasted_iota(jnp.int32, (B, B), 0)
    c_i = lax.broadcasted_iota(jnp.int32, (B, B), 1)
    earlier = jnp.where(r_i < c_i, 1.0, 0.0).astype(BF16)

    def spread_of(n, members):
        row = lax.broadcasted_iota(jnp.int32, (n, B), 0)
        row_e = lax.shift_right_logical(row, 3) // members
        at0 = jnp.where(ids[0:1, :] == row_e, 1.0, 0.0).astype(F32)
        at1 = jnp.where(ids[1:2, :] == row_e, 1.0, 0.0).astype(F32)
        named = at0 + at1
        before = jnp.dot(named.astype(BF16), earlier, preferred_element_type=F32)
        return jnp.where(before.astype(jnp.int32) == (row & 7), named, 0.0), at0, at1

    spread_t = spread_of(E * CP, 1)[0].astype(BF16)

    sc = rms_scale(shortcut[...].astype(F32))
    for q in range(NQ):
        mine = pl.ds(pl.multiple_of(c * Dh + q * kc, kc), kc)
        moe_q = (shortcut[:, mine].astype(F32) * sc * mgain[:, mine]).astype(BF16)
        buf = jnp.dot(spread_t, moe_q, preferred_element_type=F32)
        disp[q] = buf.reshape(E, CP, kc).astype(BF16)

    hid = hidden[...].astype(F32)
    ag[p] = (hid * rms_scale(hid) * dgain[...]).astype(BF16)

    real = pl.ds(0, CAP)

    def di_copy(k, q, src):
        to = lax.rem(p + k, np_)
        return pltpu.make_async_remote_copy(
            src_ref=disp.at[q, to // members, real], dst_ref=land.at[c, q, src, real],
            send_sem=di_s.at[q, k], recv_sem=di_r.at[q, src], device_id=(to, t),
            device_id_type=MESH,
        )

    def ag_copy(k, src):
        return pltpu.make_async_remote_copy(
            src_ref=ag.at[src], dst_ref=ag.at[src], send_sem=ag_s.at[k],
            recv_sem=ag_r.at[src], device_id=(lax.rem(p + k, np_), t), device_id_type=MESH,
        )

    def mate_copy(src, dst, send, recv):
        return pltpu.make_async_remote_copy(
            src_ref=src, dst_ref=dst, send_sem=send, recv_sem=recv, device_id=(p, mate),
            device_id_type=MESH,
        )

    pl.semaphore_wait(barrier, np_ + nt - 2)
    for q in range(NQ):
        each(1, np_, lambda k: di_copy(k, q, p).start())
    each(1, np_, lambda k: ag_copy(k, p).start())

    for q in range(NQ):
        land[c, q, p] = disp[q, p // members]

    spread_m, at0, at1 = spread_of(rows, members)
    weighted = spread_m * (at0 * route[0:1, :] + at1 * route[1:2, :])
    w_hi = weighted.astype(BF16)
    w_lo = (weighted - w_hi.astype(F32)).astype(BF16)

    def spread_back(w, x):
        return lax.dot_general(w, x, (((0,), (0,)), ((), ())), preferred_element_type=F32)

    def pd_copy(q, side):
        return mate_copy(land.at[side, q], land.at[side, q], pd_s.at[q], pd_r.at[q])

    nb = max(fe // 512, 1)
    cb = fe // nb
    for k in range(nk):
        q = k % NQ
        if k < NQ:
            each(1, np_, lambda j: di_copy(j, q, lax.rem(p + j, np_)).wait_recv())
            pd_copy(q, c).start()
        else:
            pd_copy(q, 1 - c).wait_recv()
        xe[k] = land[half(k), q].astype(F32).reshape(rows, kc).astype(BF16)
        w_copy(k, 0).wait()
        w_copy(k, 1).wait()
        if k == 0:
            accg[...] = jnp.dot(xe[k], pool[0], preferred_element_type=F32)
            accl[...] = jnp.dot(xe[k], pool[1], preferred_element_type=F32)
        elif k < nk - 1:
            accg[...] = accg[...] + jnp.dot(xe[k], pool[2 * k], preferred_element_type=F32)
            accl[...] = accl[...] + jnp.dot(xe[k], pool[2 * k + 1], preferred_element_type=F32)
        else:
            for b in range(nb):
                cols = slice(b * cb, (b + 1) * cb)
                g = accg[:, cols] + jnp.dot(xe[k], pool[2 * k, :, cols], preferred_element_type=F32)
                v = accl[:, cols] + jnp.dot(xe[k], pool[2 * k + 1, :, cols], preferred_element_type=F32)
                inner_e[:, cols] = silu_mul(g, v)
        if reuse and k == 0:
            for i in range(nk):
                d_copy(i, 0).start()
                d_copy(i, 1).start()
        if reuse and k == 1:
            for i in range(2):
                dd_copy(i).start()

    nh = np_ * h
    me = c if sp == 2 else 0
    each(1, np_, lambda k: ag_copy(k, lax.rem(p + k, np_)).wait_recv())
    for s in range(np_):
        stage[s * h : (s + 1) * h, :] = ag[s].astype(F32)
    mine = pl.ds(pl.multiple_of(me * nh, nh), nh)
    theirs = pl.ds(pl.multiple_of((sp - 1 - me) * nh, nh), nh)
    xd[mine, :] = stage[...].astype(BF16)
    if sp == 2:
        px = mate_copy(xd.at[mine], xd.at[mine], px_s.at[0], px_r.at[0])
        px.start()

    def pr_copy(q):
        return mate_copy(rs.at[q], rsland.at[q], pr_s.at[q], pr_r.at[q])

    def re_copy(k, q, src):
        to = lax.rem(p + k, np_)
        return pltpu.make_async_remote_copy(
            src_ref=ret.at[q, to, real], dst_ref=retland.at[q, src, real],
            send_sem=re_s.at[q, k], recv_sem=re_r.at[q, src], device_id=(to, t),
            device_id_type=MESH,
        )

    for i in range(nk):
        q = i % NQ
        e_copy(i).wait()
        o = jnp.dot(inner_e[...], epool[i], preferred_element_type=F32)
        if i < NQ:
            rs[q] = o.reshape(np_, CP, kc).astype(BF16)
            pr_copy(q).start()
        else:
            pr_copy(q).wait_recv()
            ret[q] = (o.reshape(np_, CP, kc) + rsland[q].astype(F32)).astype(BF16)
            each(1, np_, lambda k: re_copy(k, q, p).start())
            retland[q, p] = ret[q, p]

    if sp == 2:
        mate_copy(xd.at[theirs], xd.at[theirs], px_s.at[0], px_r.at[0]).wait_recv()
    for k in range(nk):
        d_copy(k, 0).wait()
        d_copy(k, 1).wait()
    g = v = None
    for k in range(nk):
        lhs = xd[:, k * kc : (k + 1) * kc]
        gk = jnp.dot(lhs, dense_w(k, 0)[...], preferred_element_type=F32)
        vk = jnp.dot(lhs, dense_w(k, 1)[...], preferred_element_type=F32)
        g = gk if g is None else g + gk
        v = vk if v is None else v + vk
    inner_d[...] = silu_mul(g, v)

    def po_copy(i):
        return mate_copy(part.at[i], pland.at[i], po_s.at[i], po_r.at[i])

    def ds_copy(k, i, src):
        to = lax.rem(p + k, np_)
        return pltpu.make_async_remote_copy(
            src_ref=ds.at[i, to], dst_ref=dland.at[i, src], send_sem=ds_s.at[i, k],
            recv_sem=ds_r.at[i, src], device_id=(to, t), device_id_type=MESH,
        )

    for i in range(2):
        dd_copy(i).wait()
        o = jnp.dot(inner_d[...], dense_d(i)[...], preferred_element_type=F32)
        if sp == 2:
            own[i] = jnp.where(c == 0, o[:nh], o[nh:])
            part[i] = jnp.where(c == 0, o[nh:], o[:nh]).astype(BF16)
            po_copy(i).start()
        else:
            own[i] = o
    for i in range(2):
        o = own[i]
        if sp == 2:
            po_copy(i).wait_recv()
            o = o + pland[i].astype(F32)
        for s in range(np_):
            ds[i, s] = o[s * h : (s + 1) * h, :].astype(BF16)
        each(1, np_, lambda k: ds_copy(k, i, p).start())
        dland[i, p] = ds[i, p]

    def fi_copy(j, q, src):
        to = lax.rem(t + j, nt)
        return pltpu.make_async_remote_copy(
            src_ref=fin.at[to, q], dst_ref=finland.at[src, q], send_sem=fi_s.at[j, q],
            recv_sem=fi_r.at[src, q], device_id=(p, to), device_id_type=MESH,
        )

    for q in range(NQ):
        each(1, np_, lambda k: re_copy(k, q, lax.rem(p + k, np_)).wait_recv())
        back = retland[q].astype(F32).reshape(rows, kc).astype(BF16)
        moe = spread_back(w_hi, back) + spread_back(w_lo, back)
        for j in range(nt):
            fin[j, q] = moe[j * h : (j + 1) * h, :].astype(BF16)
        for j in range(1, nt):
            fi_copy(j, q, t).start()
        finland[t, q] = fin[t, q]

    for i in range(2):
        each(1, np_, lambda k: ds_copy(k, i, lax.rem(p + k, np_)).wait_recv())
    for q in range(NQ):
        for j in range(1, nt):
            fi_copy(j, q, lax.rem(t + j, nt)).wait_recv()
    for i in range(2):
        acc = hid[:, i * dc : (i + 1) * dc]
        for s in range(np_):
            acc = acc + dland[i, s].astype(F32)
        for q in range(NQ):
            a = acc[:, q * kc : (q + 1) * kc]
            for j in range(i, nt, 2):
                a = a + finland[j, q].astype(F32)
            out[:, i * Dh + q * kc : i * Dh + (q + 1) * kc] = a.astype(BF16)

    def sent(k):
        for q in range(NQ):
            di_copy(k, q, p).wait_send()
            re_copy(k, q, p).wait_send()
        ag_copy(k, p).wait_send()
        for i in range(2):
            ds_copy(k, i, p).wait_send()

    each(1, np_, sent)
    for q in range(NQ):
        pd_copy(q, c).wait_send()
        pr_copy(q).wait_send()
        for j in range(1, nt):
            fi_copy(j, q, t).wait_send()
    if sp == 2:
        px.wait_send()
        for i in range(2):
            po_copy(i).wait_send()


def local(np_, nt, hidden, shortcut, ids, route, dgain, mgain, dg, dl, dd, eg, el, ed):
    h, D = hidden.shape
    B = shortcut.shape[0]
    fe = eg.shape[1]
    sp = 2 if dg.shape[1] % 256 == 0 else 1
    fd = dg.shape[1] // sp
    Dh = D // 2
    kc = Dh // NQ
    nk = 2 * NQ
    reuse = nk * fd <= fe and Dh <= fe and 2 * fd <= kc
    nh = np_ * h
    rows = np_ * CP
    dma = pltpu.SemaphoreType.DMA
    vm = pltpu.VMEM
    vspec = pl.BlockSpec(memory_space=pltpu.VMEM)
    aspec = pl.BlockSpec(memory_space=pl.ANY)
    tiny = vm((8, 128), BF16)
    return pl.pallas_call(
        functools.partial(kernel, (np_, nt, sp, reuse)),
        out_shape=pltpu.VMEM((h, D), BF16),
        in_specs=[aspec] * 12,
        out_specs=vspec,
        scratch_shapes=[
            vm((h, D), BF16), vm((B, D), BF16), vm((TOP, B), jnp.int32), vm((TOP, B), F32),
            vm((1, D), F32), vm((1, D), F32),
            vm((2 * nk, kc, fe), BF16), vm((nk, fe, kc), BF16),
            tiny if reuse else vm((nk, kc, fd), BF16),
            tiny if reuse else vm((nk, kc, fd), BF16),
            tiny if reuse else vm((2, fd, Dh), BF16),
            vm((NQ, E, CP, kc), BF16), vm((2, NQ, np_, CP, kc), BF16), vm((nk, rows, kc), BF16),
            vm((rows, fe), F32), vm((rows, fe), F32), vm((rows, fe), BF16),
            vm((np_, h, D), BF16), vm((nh, D), F32), vm((sp * nh, D), BF16), vm((sp * nh, fd), BF16),
            vm((2, nh, Dh), F32), vm((2, nh, Dh), BF16), vm((2, nh, Dh), BF16),
            vm((2, np_, h, Dh), BF16), vm((2, np_, h, Dh), BF16),
            vm((NQ, np_, CP, kc), BF16), vm((NQ, np_, CP, kc), BF16),
            vm((NQ, np_, CP, kc), BF16), vm((NQ, np_, CP, kc), BF16),
            vm((nt, NQ, h, kc), BF16), vm((nt, NQ, h, kc), BF16),
            dma((6,)), dma((2 * nk,)), dma((nk,)), dma((2 * nk + 2,)),
            dma((NQ, np_)), dma((NQ, np_)), dma((NQ,)), dma((NQ,)), dma((np_,)), dma((np_,)),
            dma((1,)), dma((1,)),
            dma((NQ,)), dma((NQ,)), dma((NQ, np_)), dma((NQ, np_)), dma((2,)), dma((2,)),
            dma((2, np_)), dma((2, np_)), dma((nt, NQ)), dma((nt, NQ)),
        ],
        compiler_params=pltpu.CompilerParams(
            collective_id=0, has_side_effects=True, vmem_limit_bytes=64 * 1024 * 1024 - 262144
        ),
    )(hidden, shortcut, ids.T, route.T, dgain.reshape(1, D), mgain.reshape(1, D), dg, dl, dd, eg, el, ed)


def solution(mesh):
    in_specs = (
        P(("dp", "tensor"), None),
        P("dp", None),
        P("dp", None),
        P("dp", None),
        P(),
        P(),
        P(None, "dp"),
        P(None, "dp"),
        P("dp", None),
        P(None, ("dp", "tensor")),
        P(None, ("dp", "tensor")),
        P(("dp", "tensor"), None),
    )
    body = functools.partial(local, mesh.shape["dp"], mesh.shape["tensor"])
    return jax.shard_map(
        body, mesh=mesh, in_specs=in_specs, out_specs=P(("dp", "tensor"), None), check_vma=False
    )
```
